128 devices in a mesh: mode: 4 (over y), mesh: 32 (over x, z, core).
Axes of the slice: x: 4, y: 4, z: 4, core: 2. Of those that a mesh axis runs over, the one named last changes fastest.
Arguments:
- velocity: float32 [3, 2, 64, 81920], P(None, None, 'mode', 'mesh'), may hold values from -2.1 to 2.1
- magnetic: float32 [3, 2, 64, 81920], P(None, None, 'mode', 'mesh'), may hold values from -2.1 to 2.1
- leaf_inverse: bfloat16 [64, 640, 128, 128], P('mode', 'mesh'), may hold values from -1 to 2
- leaf_coupling: bfloat16 [64, 128, 81920], P('mode', None, 'mesh'), may hold values from -0.05908203 to 0.05908203
- separator_inverse: bfloat16 [64, 4096, 128], P('mode', 'mesh'), may hold values from -1 to 2
- separator_coupling: bfloat16 [64, 4096, 128], P('mode', 'mesh'), may hold values from -0.26367188 to 0.26367188
- separator_source: float32 [2, 64, 4096], P(None, 'mode', 'mesh'), may hold values from -6 to 6
- front_rows: int32 [32, 2, 128], P('mesh'), may hold values from 0 to 127, each once within a row
Outputs:
- nonlinear: float32 [3, 2, 64, 81920], P(None, None, 'mode', 'mesh')
- azimuthal_field: float32 [2, 64, 81920], P(None, 'mode', 'mesh')
- separator_solution: float32 [2, 64, 4096], P(None, 'mode', 'mesh')
The draws below stay inside these ranges and needn't reach their ends.
Inputs may be any that keep to these rules, and one draw needn't show every extreme that they name: front_rows[p, 0] and front_rows[p, 1] each hold every number below 128 once.
All inputs are finite; a program needn't handle non-finite values.
Results may differ from the reference program's by a relative error of at most 0.015.
Values may be sent and summed in bfloat16 or wider, within the bound.
A program may use at most 128 MiB of HBM per device.

```python
import jax
import jax.numpy as jnp
from jax import lax

M = 64
NPHI = 192
NB = 128
NS = 128
ND = 2560
KB = 20
NODES = 81920
LEVELS = 5
N_MESH = 32


def draw_leaf_inverse(key, part):
    shape = (M, NODES // NB, NB, NB)
    identity = jnp.eye(NB, dtype=jnp.float32)
    values = identity + jax.random.truncated_normal(key, -4.0, 4.0, shape, jnp.float32) * (0.5 / NB ** 0.5)
    return values.astype(jnp.bfloat16)


def draw_separator_inverse(key, part):
    shape = (M, N_MESH, NS, NS)
    identity = jnp.eye(NS, dtype=jnp.float32)
    values = identity + jax.random.truncated_normal(key, -4.0, 4.0, shape, jnp.float32) * (0.5 / NS ** 0.5)
    return values.reshape(M, N_MESH * NS, NS).astype(jnp.bfloat16)


def steps_of(key, extent, shards, least, largest):
    def one(axis_at, blocks):
        heights = jax.random.uniform(jax.random.fold_in(jax.random.fold_in(key, 6), axis_at), (blocks,), jnp.float32, least / len(shards), largest / len(shards))
        return jnp.repeat(jnp.exp(heights), extent[axis_at] // blocks).reshape((-1,) + (1,) * (len(extent) - axis_at - 1))

    level = one(*shards[0])
    for cut in shards[1:]:
        level = level * one(*cut)
    return level


def scatter_about(key, dims, spread, reach, pieces=(), held_as=jnp.bfloat16):
    result = jax.random.normal(key, dims, jnp.float32) * spread
    if len(pieces) > 0:
        result = steps_of(key, dims, pieces, -0.22, 0.18) * result
    return jnp.clip(result, min=-reach, max=reach).astype(held_as)


def setup_inputs(seed: int = 0) -> dict:
    arg_keys = jax.random.split(jax.random.key(seed), 9)
    return {
        "velocity": scatter_about(arg_keys[0], (3, 2, M, NODES), 0.35, 2.1, ((2, 4), (3, 32)), jnp.float32),
        "magnetic": scatter_about(arg_keys[1], (3, 2, M, NODES), 0.35, 2.1, ((2, 4), (3, 32)), jnp.float32),
        "leaf_inverse": draw_leaf_inverse(jax.random.fold_in(arg_keys[8], 71), 0),
        "leaf_coupling": scatter_about(arg_keys[3], (M, NS, NODES), (0.5 * ND ** -0.5), 0.05908203, ((0, 4), (2, 32))),
        "separator_inverse": draw_separator_inverse(jax.random.fold_in(arg_keys[8], 71), 0),
        "separator_coupling": scatter_about(arg_keys[5], (M, N_MESH * NS, NS), (0.5 * NS ** -0.5), 0.26367188, ((0, 4), (1, 32))),
        "separator_source": scatter_about(arg_keys[6], (2, M, N_MESH * NS), 1.0, 6.0, ((1, 4), (2, 32)), jnp.float32),
        "front_rows": jax.vmap(lambda own: jax.random.permutation(own, NS))(jax.random.split(arg_keys[7], N_MESH * 2)).reshape((N_MESH, 2, NS)).astype(jnp.int32),
    }


highest = lax.Precision.HIGHEST
dt_step = 0.5


def tables():
    angles = jnp.arange(NPHI, dtype=jnp.int32)[:, None]
    orders = jnp.arange(M, dtype=jnp.int32)[None, :]
    phase = ((angles * orders) % NPHI).astype(jnp.float32) * (2.0 * jnp.pi / NPHI)
    forward = jnp.stack([jnp.cos(phase), jnp.sin(phase)], axis=1)
    weights = jnp.where(orders == 0, 1.0, 2.0).astype(jnp.float32) / NPHI
    backward = jnp.stack([(jnp.cos(phase) * weights).T, (jnp.sin(phase) * weights).T], axis=0)
    return forward, backward


def cross_terms(first, second):
    return jnp.stack([first[1] * second[2] - first[2] * second[1],
                      first[2] * second[0] - first[0] * second[2],
                      first[0] * second[1] - first[1] * second[0]])


def transform(forward, backward, velocity, magnetic):
    phys_velocity = jnp.einsum("kam,camn->ckn", forward, velocity, precision=highest)
    phys_magnetic = jnp.einsum("kam,camn->ckn", forward, magnetic, precision=highest)
    crossed = cross_terms(phys_velocity, phys_magnetic)
    return jnp.einsum("amk,ckn->camn", backward, crossed, precision=highest)


def rounded(values):
    return lax.optimization_barrier(values.astype(jnp.bfloat16)).astype(jnp.float32)


def forward_apply(matrix, vector):
    return jnp.einsum("mij,cmj->cmi", matrix.astype(jnp.float32), vector.astype(jnp.float32))


def transpose_apply(matrix, vector):
    return jnp.einsum("mij,cmi->cmj", matrix.astype(jnp.float32), vector.astype(jnp.float32))


def block_apply(factor, vector, form):
    shaped = vector.astype(jnp.float32).reshape(2, M, -1, NB)
    return jnp.einsum(form, factor.astype(jnp.float32), shaped).reshape(2, M, -1)


def level_of(owner):
    if owner == 0:
        return LEVELS + 1
    return (owner & -owner).bit_length()


def reference(velocity, magnetic, leaf_inverse, leaf_coupling, separator_inverse, separator_coupling, separator_source, front_rows):
    forward, backward = tables()
    pieces_out = []
    for block in range(N_MESH):
        node_span = slice(block * ND, (block + 1) * ND)
        pieces_out.append(transform(forward, backward, velocity[..., node_span], magnetic[..., node_span]))
    nonlinear = jnp.concatenate(pieces_out, axis=3)
    source = (magnetic[1] + dt_step * nonlinear[1]).astype(jnp.bfloat16)

    def leaf_parts(block):
        node_span = slice(block * ND, (block + 1) * ND)
        factor = leaf_inverse[:, block * KB:(block + 1) * KB]
        leaf_map = jnp.take(leaf_coupling[:, :, node_span], front_rows[block, 0], axis=1)
        return node_span, factor, leaf_map

    leaf_solved = []
    leaf_updates = []
    for block in range(N_MESH):
        node_span, factor, leaf_map = leaf_parts(block)
        solved = block_apply(factor, source[:, :, node_span], "mkij,cmkj->cmki").astype(jnp.bfloat16)
        leaf_solved.append(solved)
        leaf_updates.append(forward_apply(leaf_map, solved))

    def separator_parts(owner):
        row_span = slice(owner * NS, (owner + 1) * NS)
        inverse = separator_inverse[:, row_span]
        upward = jnp.take(separator_coupling[:, row_span], front_rows[owner, 1], axis=1)
        return inverse, upward, separator_source[:, :, row_span]

    reduced = {}
    outgoing = {}
    for height in range(1, LEVELS + 2):
        for owner in range(N_MESH):
            if level_of(owner) != height:
                continue
            if height == 1:
                arrived = leaf_updates[owner - 1] + leaf_updates[owner]
            elif height <= LEVELS:
                gap = 2 ** (height - 2)
                arrived = outgoing[owner - gap] + outgoing[owner + gap]
            else:
                arrived = outgoing[N_MESH // 2]
            inverse, upward, source_part = separator_parts(owner)
            reduced[owner] = forward_apply(inverse, rounded(source_part - arrived)).astype(jnp.bfloat16)
            outgoing[owner] = forward_apply(upward, reduced[owner])

    solution = {}
    inverse, upward, source_part = separator_parts(0)
    solution[0] = transpose_apply(inverse, reduced[0])
    for height in range(LEVELS, 0, -1):
        for owner in range(N_MESH):
            if level_of(owner) != height:
                continue
            if height == LEVELS:
                parent = 0
            else:
                parent = ((owner >> (height + 1)) << (height + 1)) + 2 ** height
            inverse, upward, source_part = separator_parts(owner)
            residue = reduced[owner].astype(jnp.float32) - transpose_apply(upward, rounded(solution[parent]))
            solution[owner] = transpose_apply(inverse, rounded(residue))
    separator_solution = jnp.concatenate([solution[owner] for owner in range(N_MESH)], axis=2)

    azimuthal = []
    for block in range(N_MESH):
        node_span, factor, leaf_map = leaf_parts(block)
        parent = 2 * (block // 2) + 1
        residue = leaf_solved[block].astype(jnp.float32) - transpose_apply(leaf_map, rounded(solution[parent]))
        azimuthal.append(block_apply(factor, rounded(residue), "mkji,cmkj->cmki"))
    azimuthal_field = jnp.concatenate(azimuthal, axis=2)
    return nonlinear, azimuthal_field, separator_solution
```

```python
import jax
import jax.numpy as jnp
import numpy as np
from jax import lax
from jax.experimental import pallas as pl
from jax.experimental.pallas import tpu as pltpu
from jax.sharding import PartitionSpec as P

M = 64
NPHI = 192
DT = 0.5
MESH = pl.DeviceIdType.MESH
F32 = jnp.float32
BF16 = jnp.bfloat16

SLOT_OF = ((0, 0), (0, 2), (1, 0), (1, 2), (0, 1), (1, 1))
VR, VZ, BR, BZ, VP, BP = range(6)


def tables(parts):
    local = M // parts
    k = np.arange(NPHI)[:, None]
    m = np.arange(M)[None, :]
    phase = ((k * m) % NPHI) * (2.0 * np.pi / NPHI)
    both = np.stack([np.cos(phase), np.sin(phase)])
    both = both.reshape(2, NPHI, parts, local).transpose(1, 2, 0, 3).reshape(NPHI, 2 * M)
    weights = np.where(np.arange(M) == 0, 1.0, 2.0) / NPHI
    w = np.broadcast_to(weights.reshape(parts, 1, local), (parts, 2, local)).reshape(2 * M)
    return jnp.asarray(both, BF16), jnp.asarray((both * w).T, BF16)


def dot(a, b):
    return jnp.dot(a, b, preferred_element_type=F32)


def dot_nt(a, b):
    return lax.dot_general(a, b, (((1,), (1,)), ((), ())), preferred_element_type=F32)


def level_of(q, levels):
    return levels + 1 if q == 0 else (q & -q).bit_length()


def parent_of(q, levels):
    level = level_of(q, levels)
    if level == levels:
        return 0
    return (q >> (level + 1) << (level + 1)) + 2**level


def kernel(
    parts, places,
    vel, mag, linv, lcpl, sinv, scpl, ssrc, rows, tab_f, tab_b,
    nl_out, az_out, sol_out,
    stage, vb, xr, tf, tb, nb, nr, nl32, src16, lin, gup, smat, cmat, hmat, ssv, rowv, pt0, p1,
    srcb, ubuf, urow, hs, ss, srcs, us, xo, xin, ls, az, sol,
    sem_vb, sem_tab, sem_small, sem_lin, sem_g, sem_s1, sem_r1, sem_own, sem_s2, sem_r2, sem_own2,
    sem_ss, sem_sh, sem_sc, sem_rs, sem_rh, sem_rc, sem_us, sem_ur, sem_xs, sem_xr, sem_out,
):
    modes = src16.shape[0] // 2
    nodes = src16.shape[1]
    chunk = nodes // parts
    blocks = lin.shape[1]
    levels = places.bit_length() - 1
    y = lax.axis_index("mode")
    me = lax.axis_index("mesh")
    solver = lax.rem(me, 2) == 1

    def lanes_of(part):
        return pl.ds(pl.multiple_of(part * chunk, 128), chunk)

    def drain(ref, sem):
        pltpu.make_async_copy(ref, ref, sem).wait()

    for slot, (which, comp) in enumerate(SLOT_OF):
        pltpu.make_async_copy((vel, mag)[which].at[comp], stage.at[slot], sem_vb.at[slot]).start()
    small = ((sinv, smat), (scpl, cmat), (ssrc, ssv), (rows, rowv), (tab_f, tf), (tab_b, tb))
    for i, (a, b) in enumerate(small):
        pltpu.make_async_copy(a, b, sem_small.at[i]).start()

    def load_mode(m, carry):
        pltpu.make_async_copy(linv.at[m], lin.at[m], sem_lin.at[m]).start()
        pltpu.make_async_copy(lcpl.at[m], gup.at[m], sem_g.at[m]).start()
        return carry

    lax.fori_loop(0, modes, load_mode, 0)

    barrier = pltpu.get_barrier_semaphore()

    def greet(i, carry):
        other = lax.rem(me + i, places)
        pl.semaphore_signal(barrier, inc=1, device_id=(y, other), device_id_type=MESH)
        return carry

    for d in range(1, parts):
        pl.semaphore_signal(barrier, inc=1, device_id=(lax.rem(y + d, parts), me), device_id_type=MESH)
    lax.fori_loop(1, places, greet, 0)

    for slot in range(4):
        drain(stage.at[slot], sem_vb.at[slot])
        vb[slot] = stage[slot].astype(BF16)
    pl.semaphore_wait(barrier, parts - 1 + places - 1)

    def exchange(group, lo, hi):
        for d in range(1, parts):
            other = lax.rem(y + d, parts)
            pltpu.make_async_remote_copy(
                src_ref=vb.at[lo:hi, :, :, lanes_of(other)], dst_ref=xr.at[lo:hi, y],
                send_sem=sem_s1.at[group, d - 1], recv_sem=sem_r1.at[group, d - 1],
                device_id=(other, me), device_id_type=MESH,
            ).start()
        pltpu.make_async_copy(vb.at[lo:hi, :, :, lanes_of(y)], xr.at[lo:hi, y], sem_own.at[group]).start()

    def exchanged(group, lo, hi):
        for d in range(1, parts):
            drain(xr.at[lo:hi, 0], sem_r1.at[group, d - 1])
        drain(xr.at[lo:hi, 0], sem_own.at[group])

    exchange(0, 0, 4)
    for slot in range(4, 6):
        drain(stage.at[slot], sem_vb.at[slot])
        vb[slot] = stage[slot].astype(BF16)

    for i, (a, b) in enumerate(small):
        drain(b, sem_small.at[i])

    def for_solvers(act, own):
        def one(m, carry):
            there = 2 * m + 1
            pl.when(there != me)(lambda: act(m, there))
            pl.when(there == me)(lambda: own(m))
            return carry

        lax.fori_loop(0, modes, one, 0)

    def remote(src, dst, send, recv, there):
        return pltpu.make_async_remote_copy(
            src_ref=src, dst_ref=dst, send_sem=send, recv_sem=recv, device_id=(y, there), device_id_type=MESH
        )

    srow = lax.broadcasted_iota(jnp.int32, (128, 128), 0)
    pt0[...] = (srow == jnp.broadcast_to(rowv[0, 0:1, :], (128, 128))).astype(F32).astype(BF16)
    p1[...] = (srow == jnp.broadcast_to(rowv[0, 1:2, :], (128, 128))).astype(F32).T.astype(BF16)

    def build_h(m, carry):
        coupling = dot(p1[...], cmat[m]).astype(BF16)
        hmat[m] = dot(coupling, smat[m]).astype(BF16)
        return carry

    lax.fori_loop(0, modes, build_h, 0, unroll=4)
    srcb[...] = jnp.zeros_like(srcb)
    ubuf[...] = jnp.zeros_like(ubuf)
    for m in range(modes):
        for c in range(2):
            srcb[m, c : c + 1, :] = ssv[c, m : m + 1, :]
    for_solvers(
        lambda m, t: remote(hmat.at[m], hs.at[me], sem_sh.at[m], sem_rh, t).start(),
        lambda m: pltpu.make_async_copy(hmat.at[m], hs.at[me], sem_rh).start(),
    )
    for_solvers(
        lambda m, t: remote(srcb.at[m], srcs.at[me], sem_sc.at[m], sem_rc, t).start(),
        lambda m: pltpu.make_async_copy(srcb.at[m], srcs.at[me], sem_rc).start(),
    )
    for_solvers(
        lambda m, t: remote(smat.at[m], ss.at[me], sem_ss.at[m], sem_rs, t).start(),
        lambda m: pltpu.make_async_copy(smat.at[m], ss.at[me], sem_rs).start(),
    )

    def build_g(m, carry):
        drain(lin.at[m], sem_lin.at[m])
        drain(gup.at[m], sem_g.at[m])
        for b in range(blocks):
            at = slice(b * 128, (b + 1) * 128)
            gup[m, :, at] = dot(gup[m, :, at], lin[m, b]).astype(BF16)
        return carry

    lax.fori_loop(0, modes, build_g, 0)

    def transform(jobs):
        at = 0
        while at < chunk:
            width = min(256, chunk - at)
            here = slice(at, at + width)
            need = sorted({s for _, pairs in jobs for s in pairs})
            phys = {s: dot(tf[...], xr[s, :, :, :, here].reshape(2 * M, width)) for s in need}
            for comp, (a, b, c, d) in jobs:
                crossed = phys[a] * phys[b] - phys[c] * phys[d]
                back = dot(tb[...], crossed.astype(BF16)).astype(BF16)
                nb[comp, :, :, :, here] = back.reshape(parts, 2, modes, width)
            at += width

    def give_back(group, comp):
        for d in range(1, parts):
            other = lax.rem(y + d, parts)
            pltpu.make_async_remote_copy(
                src_ref=nb.at[comp, other], dst_ref=nr.at[comp, :, :, lanes_of(y)],
                send_sem=sem_s2.at[group, d - 1], recv_sem=sem_r2.at[group, d - 1],
                device_id=(other, me), device_id_type=MESH,
            ).start()
        pltpu.make_async_copy(nb.at[comp, y], nr.at[comp, :, :, lanes_of(y)], sem_own2.at[group]).start()

    def given_back(group, comp):
        for d in range(1, parts):
            drain(nb.at[comp, 0], sem_r2.at[group, d - 1])
        drain(nb.at[comp, 0], sem_own2.at[group])

    exchanged(0, 0, 4)
    transform([(1, (VZ, BR, VR, BZ))])
    give_back(0, 1)
    exchange(1, 4, 6)

    given_back(0, 1)
    phi = nr[1].astype(F32)
    nl32[1] = phi
    source = stage[BP] + DT * phi
    src16[...] = source.astype(BF16).reshape(2 * modes, nodes)
    pltpu.make_async_copy(nl32.at[1], nl_out.at[1], sem_out.at[0]).start()

    mode_of = lax.rem(lax.broadcasted_iota(jnp.int32, (2 * modes, 128), 0), modes)

    def update(m, acc):
        return jnp.where(mode_of == m, dot_nt(src16[...], gup[m]), acc)

    leaf_update = lax.fori_loop(0, modes, update, jnp.zeros((2 * modes, 128), F32), unroll=4)
    urow[...] = dot(leaf_update.astype(BF16), pt0[...])
    for m in range(modes):
        for c in range(2):
            ubuf[m, c : c + 1, :] = urow[c * modes + m : c * modes + m + 1, :]
    for_solvers(
        lambda m, t: remote(ubuf.at[m], us.at[me], sem_us.at[m], sem_ur, t).start(),
        lambda m: pltpu.make_async_copy(ubuf.at[m], us.at[me], sem_ur).start(),
    )

    exchanged(1, 4, 6)
    transform([(0, (VP, BZ, VZ, BP)), (2, (VR, BP, VP, BR))])
    give_back(1, 0)
    give_back(2, 2)

    def leaf_forward(m, carry):
        for b in range(blocks):
            at = slice(b * 128, (b + 1) * 128)
            ls[:, at] = jnp.where(mode_of == m, dot_nt(src16[:, at], lin[m, b]), ls[:, at])
        return carry

    ls[...] = jnp.zeros_like(ls)
    lax.fori_loop(0, modes, leaf_forward, 0)

    @pl.when(solver)
    def _():
        drain(hs, sem_rh)
        drain(srcs, sem_rc)
        drain(us, sem_ur)
        drain(ss, sem_rs)
        out, w = {}, {}
        order = sorted(range(places), key=lambda q: level_of(q, levels))
        for q in order:
            level = level_of(q, levels)
            if level == 1:
                arrived = us[q - 1] + us[q]
            elif level <= levels:
                gap = 2 ** (level - 2)
                arrived = out[q - gap] + out[q + gap]
            else:
                arrived = out[places // 2]
            g = (srcs[q] - arrived).astype(BF16)
            if level <= levels:
                out[q] = dot_nt(g, hs[q])
            reduced = dot_nt(g, ss[q]).astype(BF16)
            w[q] = dot(reduced, ss[q])
        x = {0: w[0]}
        for q in order[::-1][1:]:
            x[q] = w[q] - dot(x[parent_of(q, levels)].astype(BF16), hs[q])
        first = lax.broadcasted_iota(jnp.int32, (8, 128), 0) < 2
        for p in range(places):
            xo[p] = jnp.where(first, x[p], pltpu.roll(x[2 * (p // 2) + 1], 2, 0))

        def send(p, carry):
            def away():
                pltpu.make_async_remote_copy(
                    src_ref=xo.at[p], dst_ref=xin.at[lax.div(me, 2)], send_sem=sem_xs.at[p], recv_sem=sem_xr,
                    device_id=(y, p), device_id_type=MESH,
                ).start()

            pl.when(p != me)(away)
            pl.when(p == me)(lambda: pltpu.make_async_copy(xo.at[p], xin.at[lax.div(me, 2)], sem_xr).start())
            return carry

        lax.fori_loop(0, places, send, 0)

    def leaf_back(b, carry):
        at = pl.ds(pl.multiple_of(b * 128, 128), 128)
        own = ls[:, at].astype(BF16)
        acc = jnp.zeros((2 * modes, 128), F32)
        for m in range(modes):
            acc = jnp.where(mode_of == m, dot(own, lin[m, b]), acc)
        az[:, at] = acc
        return carry

    lax.fori_loop(0, blocks, leaf_back, 0)

    given_back(1, 0)
    given_back(2, 2)
    nl32[0] = nr[0].astype(F32)
    nl32[2] = nr[2].astype(F32)
    pltpu.make_async_copy(nl32.at[0], nl_out.at[0], sem_out.at[1]).start()
    pltpu.make_async_copy(nl32.at[2], nl_out.at[2], sem_out.at[2]).start()

    drain(xin, sem_xr)
    for m in range(modes):
        for c in range(2):
            sol[c, m : m + 1, :] = xin[m, c : c + 1, :]
            urow[c * modes + m : c * modes + m + 1, :] = xin[m, 2 + c : 3 + c, :]
    pltpu.make_async_copy(sol, sol_out, sem_out.at[3]).start()
    above = dot_nt(urow[...].astype(BF16), pt0[...]).astype(BF16)

    def finish(m, carry):
        mine = jnp.where(mode_of == m, above, jnp.zeros_like(above))
        az[...] -= dot(mine, gup[m])
        return carry

    lax.fori_loop(0, modes, finish, 0, unroll=2)
    pltpu.make_async_copy(az, az_out, sem_out.at[4]).start()

    for group, (lo, hi) in enumerate(((0, 4), (4, 6))):
        for d in range(1, parts):
            drain(xr.at[lo:hi, 0], sem_s1.at[group, d - 1])
    for group in range(3):
        for d in range(1, parts):
            drain(nb.at[0, 0], sem_s2.at[group, d - 1])

    def sent(m, carry):
        @pl.when(2 * m + 1 != me)
        def _():
            drain(hmat.at[m], sem_sh.at[m])
            drain(smat.at[m], sem_ss.at[m])
            drain(srcb.at[m], sem_sc.at[m])
            drain(ubuf.at[m], sem_us.at[m])

        return carry

    lax.fori_loop(0, modes, sent, 0)

    @pl.when(solver)
    def _():
        def one(p, carry):
            pl.when(p != me)(lambda: drain(xo.at[p], sem_xs.at[p]))
            return carry

        lax.fori_loop(0, places, one, 0)

    for i, ref in enumerate((nl32.at[1], nl32.at[0], nl32.at[2], sol, az)):
        drain(ref, sem_out.at[i])


def solution(mesh):
    parts, places = mesh.shape["mode"], mesh.shape["mesh"]
    in_specs = (
        P(None, None, "mode", "mesh"),
        P(None, None, "mode", "mesh"),
        P("mode", "mesh", None, None),
        P("mode", None, "mesh"),
        P("mode", "mesh", None),
        P("mode", "mesh", None),
        P(None, "mode", "mesh"),
        P("mesh", None, None),
    )
    out_specs = (P(None, None, "mode", "mesh"), P(None, "mode", "mesh"), P(None, "mode", "mesh"))

    def shards(vel, mag, linv, lcpl, sinv, scpl, ssrc, rows):
        modes, nodes = vel.shape[2], vel.shape[3]
        blocks = linv.shape[1]
        chunk = nodes // parts
        tab_f, tab_b = tables(parts)
        vm = pltpu.VMEM
        dma = pltpu.SemaphoreType.DMA
        scratch = [
            vm((6, 2, modes, nodes), F32),
            vm((6, 2, modes, nodes), BF16),
            vm((6, parts, 2, modes, chunk), BF16),
            vm((NPHI, 2 * M), BF16),
            vm((2 * M, NPHI), BF16),
            vm((3, parts, 2, modes, chunk), BF16),
            vm((3, 2, modes, nodes), BF16),
            vm((3, 2, modes, nodes), F32),
            vm((2 * modes, nodes), BF16),
            vm((modes, blocks, 128, 128), BF16),
            vm((modes, 128, nodes), BF16),
            vm((modes, 128, 128), BF16),
            vm((modes, 128, 128), BF16),
            vm((modes, 128, 128), BF16),
            vm((2, modes, 128), F32),
            vm((1, 2, 128), jnp.int32),
            vm((128, 128), BF16),
            vm((128, 128), BF16),
            vm((modes, 8, 128), F32),
            vm((modes, 8, 128), F32),
            vm((2 * modes, 128), F32),
            vm((places, 128, 128), BF16),
            vm((places, 128, 128), BF16),
            vm((places, 8, 128), F32),
            vm((places, 8, 128), F32),
            vm((places, 8, 128), F32),
            vm((modes, 8, 128), F32),
            vm((2 * modes, nodes), F32),
            vm((2 * modes, nodes), F32),
            vm((2, modes, 128), F32),
            dma((6,)), dma((1,)), dma((6,)), dma((modes,)), dma((modes,)),
            dma((2, parts - 1)), dma((2, parts - 1)), dma((2,)),
            dma((3, parts - 1)), dma((3, parts - 1)), dma((3,)),
            dma((modes,)), dma((modes,)), dma((modes,)), dma, dma, dma,
            dma((modes,)), dma, dma((places,)), dma, dma((5,)),
        ]
        any_spec = pl.BlockSpec(memory_space=pl.ANY)

        def body(*refs):
            kernel(parts, places, *refs)

        nl, az, sol = pl.pallas_call(
            body,
            name="dynamo",
            out_shape=(
                jax.ShapeDtypeStruct((3, 2, modes, nodes), F32),
                jax.ShapeDtypeStruct((2 * modes, nodes), F32),
                jax.ShapeDtypeStruct((2, modes, 128), F32),
            ),
            in_specs=[any_spec] * 10,
            out_specs=(any_spec,) * 3,
            scratch_shapes=scratch,
            compiler_params=pltpu.CompilerParams(
                collective_id=0, has_side_effects=True, vmem_limit_bytes=60 * 2**20
            ),
        )(vel, mag, linv, lcpl, sinv, scpl, ssrc, rows, tab_f, tab_b)
        return nl, az.reshape(2, modes, nodes), sol

    return jax.shard_map(shards, mesh=mesh, in_specs=in_specs, out_specs=out_specs, check_vma=False)
```

```python
import jax
import jax.numpy as jnp
import numpy as np
from jax import lax
from jax.experimental import pallas as pl
from jax.experimental.pallas import tpu as pltpu
from jax.sharding import PartitionSpec as P

M = 64
NPHI = 192
DT = 0.5
MESH = pl.DeviceIdType.MESH
F32 = jnp.float32
BF16 = jnp.bfloat16

SLOT_OF = ((0, 0), (0, 2), (1, 0), (1, 2), (0, 1), (1, 1))
VR, VZ, BR, BZ, VP, BP = range(6)


def tables(parts):
    local = M // parts
    k = np.arange(NPHI)[:, None]
    m = np.arange(M)[None, :]
    phase = ((k * m) % NPHI) * (2.0 * np.pi / NPHI)
    both = np.stack([np.cos(phase), np.sin(phase)])
    both = both.reshape(2, NPHI, parts, local).transpose(1, 2, 0, 3).reshape(NPHI, 2 * M)
    weights = np.where(np.arange(M) == 0, 1.0, 2.0) / NPHI
    w = np.broadcast_to(weights.reshape(parts, 1, local), (parts, 2, local)).reshape(2 * M)
    return jnp.asarray(both, BF16), jnp.asarray((both * w).T, BF16)


def dot(a, b):
    return jnp.dot(a, b, preferred_element_type=F32)


def dot_nt(a, b):
    return lax.dot_general(a, b, (((1,), (1,)), ((), ())), preferred_element_type=F32)


def level_of(q, levels):
    return levels + 1 if q == 0 else (q & -q).bit_length()


def parent_of(q, levels):
    level = level_of(q, levels)
    if level == levels:
        return 0
    return (q >> (level + 1) << (level + 1)) + 2**level


def kernel(
    parts, places,
    vel, mag, linv, lcpl, sinv, scpl, ssrc, rows, tab_f, tab_b,
    nl32, az, sol,
    stage, vb, xr, tf, tb, nb, nr, src16, lin, gup, smat, cmat, hmat, ssv, rowv, pt0, p1,
    srcb, ubuf, urow, hs, ss, srcs, us, xo, xin, ls,
    sem_vb, sem_small, sem_lin, sem_g, sem_s1, sem_r1, sem_s2, sem_r2,
    sem_ss, sem_sh, sem_sc, sem_rs, sem_rh, sem_rc, sem_us, sem_ur, sem_xs, sem_xr,
):
    modes = src16.shape[0] // 2
    nodes = src16.shape[1]
    chunk = nodes // parts
    blocks = lin.shape[1]
    levels = places.bit_length() - 1
    y = lax.axis_index("mode")
    me = lax.axis_index("mesh")
    solver = lax.rem(me, 2) == 1

    def lanes_of(part):
        return pl.ds(pl.multiple_of(part * chunk, 128), chunk)

    def drain(ref, sem):
        pltpu.make_async_copy(ref, ref, sem).wait()

    for slot, (which, comp) in enumerate(SLOT_OF):
        pltpu.make_async_copy((vel, mag)[which].at[comp], stage.at[slot], sem_vb.at[slot]).start()
    barrier = pltpu.get_barrier_semaphore()

    def greet(i, carry):
        other = jnp.where(me + i >= places, me + i - places, me + i)
        pl.semaphore_signal(barrier, inc=1, device_id=(y, other), device_id_type=MESH)
        return carry

    for d in range(1, parts):
        pl.semaphore_signal(barrier, inc=1, device_id=(lax.rem(y + d, parts), me), device_id_type=MESH)
    lax.fori_loop(1, places, greet, 0)

    small = ((sinv, smat), (scpl, cmat), (ssrc, ssv), (rows, rowv), (tab_f, tf), (tab_b, tb))
    for i, (a, b) in enumerate(small):
        pltpu.make_async_copy(a, b, sem_small.at[i]).start()

    for slot in range(4):
        drain(stage.at[slot], sem_vb.at[slot])
        vb[slot] = stage[slot].astype(BF16)
    pl.semaphore_wait(barrier, parts - 1 + places - 1)

    def to_mode(src, dst, send, recv, other):
        return pltpu.make_async_remote_copy(
            src_ref=src, dst_ref=dst, send_sem=send, recv_sem=recv, device_id=(other, me), device_id_type=MESH
        )

    after, before = lax.rem(y + 1, parts), lax.rem(y + parts - 1, parts)

    def exchange(group, lo, hi):
        for d in (2, 3, 1):
            other = lax.rem(y + d, parts)
            to_mode(
                vb.at[lo:hi, :, :, lanes_of(other)], xr.at[lo:hi, y],
                sem_s1.at[group, d - 1], sem_r1.at[group, d - 1], other,
            ).start()
        for slot in range(lo, hi):
            xr[slot, y] = vb[slot, :, :, lanes_of(y)]

    def exchanged(group, lo, hi):
        for d in range(1, parts):
            drain(xr.at[lo:hi, 0], sem_r1.at[group, d - 1])

    exchange(0, 0, 4)
    def load_mode(m, carry):
        pltpu.make_async_copy(linv.at[m], lin.at[m], sem_lin.at[m]).start()
        pltpu.make_async_copy(lcpl.at[m], gup.at[m], sem_g.at[m]).start()
        return carry

    lax.fori_loop(0, modes, load_mode, 0)

    for slot in range(4, 6):
        drain(stage.at[slot], sem_vb.at[slot])
        vb[slot] = stage[slot].astype(BF16)

    for i, (a, b) in enumerate(small):
        drain(b, sem_small.at[i])

    def for_solvers(act, own):
        def one(m, carry):
            there = 2 * m + 1
            pl.when(there != me)(lambda: act(m, there))
            pl.when(there == me)(lambda: own(m))
            return carry

        lax.fori_loop(0, modes, one, 0)

    def remote(src, dst, send, recv, there):
        return pltpu.make_async_remote_copy(
            src_ref=src, dst_ref=dst, send_sem=send, recv_sem=recv, device_id=(y, there), device_id_type=MESH
        )

    for_solvers(
        lambda m, t: remote(smat.at[m], ss.at[me], sem_ss, sem_rs, t).start(),
        lambda m: pltpu.make_async_copy(smat.at[m], ss.at[me], sem_rs).start(),
    )
    srow = lax.broadcasted_iota(jnp.int32, (128, 128), 0)
    pt0[...] = (srow == jnp.broadcast_to(rowv[0, 0:1, :], (128, 128))).astype(F32).astype(BF16)
    p1[...] = (srow == jnp.broadcast_to(rowv[0, 1:2, :], (128, 128))).astype(F32).T.astype(BF16)

    def build_h(m, carry):
        coupling = dot(p1[...], cmat[m]).astype(BF16)
        hmat[m] = dot(coupling, smat[m]).astype(BF16)
        return carry

    lax.fori_loop(0, modes, build_h, 0, unroll=4)
    srcb[...] = jnp.zeros_like(srcb)
    ubuf[...] = jnp.zeros_like(ubuf)
    for m in range(modes):
        for c in range(2):
            srcb[m, c : c + 1, :] = ssv[c, m : m + 1, :]
    for_solvers(
        lambda m, t: remote(hmat.at[m], hs.at[me], sem_sh, sem_rh, t).start(),
        lambda m: pltpu.make_async_copy(hmat.at[m], hs.at[me], sem_rh).start(),
    )
    for_solvers(
        lambda m, t: remote(srcb.at[m], srcs.at[me], sem_sc, sem_rc, t).start(),
        lambda m: pltpu.make_async_copy(srcb.at[m], srcs.at[me], sem_rc).start(),
    )

    zero = jnp.zeros((128, 128), BF16)

    together = 4

    def build_g(i, carry):
        for j in range(together):
            drain(lin.at[i * together + j], sem_lin.at[i * together + j])
            drain(gup.at[i * together + j], sem_g.at[i * together + j])
        for j in range(together):
            m = i * together + j
            for b in range(0, blocks, 2):
                at = slice(b * 128, (b + 2) * 128)
                both = jnp.concatenate(
                    [jnp.concatenate([lin[m, b], zero], 1), jnp.concatenate([zero, lin[m, b + 1]], 1)], 0
                )
                gup[m, :, at] = dot(gup[m, :, at], both).astype(BF16)
        return carry

    lax.fori_loop(0, 1, build_g, 0)
    lax.fori_loop(1, modes // together, build_g, 0)

    def transform(jobs):
        at = 0
        while at < chunk:
            width = min(256, chunk - at)
            here = slice(at, at + width)
            need = sorted({s for _, pairs in jobs for s in pairs})
            phys = {s: dot(tf[...], xr[s, :, :, :, here].reshape(2 * M, width)) for s in need}
            for comp, (a, b, c, d) in jobs:
                crossed = phys[a] * phys[b] - phys[c] * phys[d]
                back = dot(tb[...], crossed.astype(BF16)).astype(BF16)
                nb[comp, :, :, :, here] = back.reshape(parts, 2, modes, width)
            at += width

    def give_back(group, comp):
        for d in (2, 3, 1):
            other = lax.rem(y + d, parts)
            to_mode(
                nb.at[comp, other], nr.at[comp, :, :, lanes_of(y)],
                sem_s2.at[group, d - 1], sem_r2.at[group, d - 1], other,
            ).start()
        nr[comp, :, :, lanes_of(y)] = nb[comp, y]

    exchanged(0, 0, 4)
    transform([(1, (VZ, BR, VR, BZ))])
    give_back(0, 1)

    mode_of = lax.rem(lax.broadcasted_iota(jnp.int32, (2 * modes, 128), 0), modes)
    leaf_update = jnp.zeros((2 * modes, 128), F32)
    for d in (0, 3, 1, 2):
        here = lanes_of(lax.rem(y + parts - d, parts))
        if d:
            drain(nb.at[1, 0], sem_r2.at[0, d - 1])
        source = stage[BP, :, :, here] + DT * nr[1, :, :, here].astype(F32)
        own = source.astype(BF16).reshape(2 * modes, chunk)
        src16[:, here] = own

        def update(m, acc, own=own, here=here):
            return acc + jnp.where(mode_of == m, dot_nt(own, gup[m, :, here]), 0.0)

        leaf_update = lax.fori_loop(0, modes, update, leaf_update, unroll=True)
        if d == 1:
            exchange(1, 4, 6)
    nl32[1] = nr[1].astype(F32)
    urow[...] = dot(leaf_update.astype(BF16), pt0[...])
    for m in range(modes):
        for c in range(2):
            ubuf[m, c : c + 1, :] = urow[c * modes + m : c * modes + m + 1, :]
    for_solvers(
        lambda m, t: remote(ubuf.at[m], us.at[me], sem_us, sem_ur, t).start(),
        lambda m: pltpu.make_async_copy(ubuf.at[m], us.at[me], sem_ur).start(),
    )

    def pair_at(b):
        return pl.ds(pl.multiple_of(b * 256, 256), 256)

    low = lax.broadcasted_iota(jnp.int32, (2 * modes, 256), 1) < 128

    def leaf_forward(b, carry):
        own = src16[:, pair_at(b)].astype(F32)
        own = jnp.concatenate([jnp.where(low, own, 0.0), jnp.where(low, 0.0, own)], 0).astype(BF16)
        left = right = jnp.zeros((2 * modes, 128), F32)
        for m in range(modes):
            got = dot_nt(own, jnp.concatenate([lin[m, 2 * b], lin[m, 2 * b + 1]], 1))
            left = jnp.where(mode_of == m, got[: 2 * modes], left)
            right = jnp.where(mode_of == m, got[2 * modes :], right)
        ls[:, pair_at(b)] = jnp.concatenate([left, right], 1).astype(BF16)
        return carry

    lax.fori_loop(0, blocks // 2, leaf_forward, 0, unroll=2)

    exchanged(1, 4, 6)
    transform([(0, (VP, BZ, VZ, BP)), (2, (VR, BP, VP, BR))])
    give_back(1, 0)
    give_back(2, 2)

    @pl.when(solver)
    def _():
        drain(hs, sem_rh)
        drain(srcs, sem_rc)
        drain(us, sem_ur)
        drain(ss, sem_rs)
        ranked = [[q for q in range(places) if level_of(q, levels) == k] for k in range(levels + 2)]
        top = places // 2
        none = jnp.zeros((2, 128), F32)

        def side(a, b):
            return jnp.concatenate([a, b], 1)

        def g_of(q, arrived):
            return srcs[q] - arrived

        joined = dot(ss[0], hs[top]).astype(BF16)
        g, w, x = {}, {}, {}
        arrived = {q: us[q - 1] + us[q] for q in ranked[1]}
        for level in range(1, levels):
            for q in ranked[level]:
                g[q] = g_of(q, arrived[q])
            for a, b in zip(ranked[level][::2], ranked[level][1::2]):
                both = side(g[a], g[b]).astype(BF16)
                arrived[(a + b) // 2] = dot_nt(both, side(hs[a], hs[b]))
            for a, b in zip(ranked[level][::2], ranked[level][1::2]):
                rows_ab = jnp.concatenate([side(g[a], none), side(none, g[b])], 0).astype(BF16)
                reduced = dot_nt(rows_ab, side(ss[a], ss[b])).astype(BF16)
                got = dot(reduced, side(ss[a], ss[b]))
                w[a], w[b] = got[:2, :128], got[2:, 128:]
        g_top = g_of(top, arrived[top]).astype(BF16)
        reduced_top = dot_nt(g_top, ss[top]).astype(BF16).astype(F32)
        reduced_0 = (dot_nt(srcs[0].astype(BF16), ss[0]) - dot_nt(g_top, joined)).astype(BF16)
        x[top] = dot(
            side(reduced_top, -reduced_0.astype(F32)).astype(BF16), jnp.concatenate([ss[top], joined], 0)
        )
        x[0] = dot(reduced_0, ss[0])
        for level in range(levels - 1, 0, -1):
            for a, b in zip(ranked[level][::2], ranked[level][1::2]):
                got = dot(x[parent_of(a, levels)].astype(BF16), side(hs[a], hs[b]))
                x[a], x[b] = w[a] - got[:, :128], w[b] - got[:, 128:]
        for p in range(places):
            xo[p, 0:2, :] = x[p]
            xo[p, 2:4, :] = x[2 * (p // 2) + 1]

        def send(p, carry):
            def away():
                pltpu.make_async_remote_copy(
                    src_ref=xo.at[p], dst_ref=xin.at[lax.div(me, 2)], send_sem=sem_xs, recv_sem=sem_xr,
                    device_id=(y, p), device_id_type=MESH,
                ).start()

            pl.when(p != me)(away)
            pl.when(p == me)(lambda: pltpu.make_async_copy(xo.at[p], xin.at[lax.div(me, 2)], sem_xr).start())
            return carry

        lax.fori_loop(0, places, send, 0)

    mode_col = jnp.concatenate([mode_of, mode_of], 0)

    def stacked(rows, which):
        rows = rows.astype(F32)
        return jnp.concatenate([jnp.where(which == m, rows, 0.0).astype(BF16) for m in range(modes)], 1)

    def leaf_back(b, carry):
        own = ls[:, pair_at(b)]
        own = stacked(jnp.concatenate([own[:, :128], own[:, 128:]], 0), mode_col)
        both = jnp.concatenate(
            [jnp.concatenate([lin[m, 2 * b], lin[m, 2 * b + 1]], 1) for m in range(modes)], 0
        )
        got = dot(own, both)
        az[:, pair_at(b)] = jnp.concatenate([got[: 2 * modes, :128], got[2 * modes :, 128:]], 1)
        return carry

    lax.fori_loop(0, blocks // 2, leaf_back, 0, unroll=5)

    for comp in (0, 2):
        for d in range(1, parts):
            drain(nb.at[comp, 0], sem_r2.at[1 + comp // 2, d - 1])
        nl32[comp] = nr[comp].astype(F32)

    for group, (lo, hi) in enumerate(((0, 4), (4, 6))):
        for d in range(1, parts):
            drain(xr.at[lo:hi, 0], sem_s1.at[group, d - 1])
    for group in range(3):
        for d in range(1, parts):
            drain(nb.at[0, 0], sem_s2.at[group, d - 1])

    def sent(count):
        drain(hmat.at[:count], sem_sh)
        drain(smat.at[:count], sem_ss)
        drain(srcb.at[:count], sem_sc)
        drain(ubuf.at[:count], sem_us)

    @pl.when(solver)
    def _():
        sent(modes - 1)
        drain(xo.at[: places - 1], sem_xs)

    pl.when(jnp.logical_not(solver))(lambda: sent(modes))

    drain(xin, sem_xr)
    for m in range(modes):
        for c in range(2):
            sol[c, m : m + 1, :] = xin[m, c : c + 1, :]
            urow[c * modes + m : c * modes + m + 1, :] = xin[m, 2 + c : 3 + c, :]
    above = dot_nt(urow[...].astype(BF16), pt0[...]).astype(BF16)

    above = stacked(above, mode_of)
    for b in range(blocks // 2):
        at = slice(b * 256, (b + 1) * 256)
        az[:, at] -= dot(above, gup[:, :, at].reshape(modes * 128, 256))


def put_out(*refs):
    moves = [pltpu.make_async_copy(refs[i], refs[3 + i], refs[6].at[i]) for i in range(3)]
    for move in moves:
        move.start()
    for move in moves:
        move.wait()


def solution(mesh):
    parts, places = mesh.shape["mode"], mesh.shape["mesh"]
    in_specs = (
        P(None, None, "mode", "mesh"),
        P(None, None, "mode", "mesh"),
        P("mode", "mesh", None, None),
        P("mode", None, "mesh"),
        P("mode", "mesh", None),
        P("mode", "mesh", None),
        P(None, "mode", "mesh"),
        P("mesh", None, None),
    )
    out_specs = (P(None, None, "mode", "mesh"), P(None, "mode", "mesh"), P(None, "mode", "mesh"))

    def shards(vel, mag, linv, lcpl, sinv, scpl, ssrc, rows):
        modes, nodes = vel.shape[2], vel.shape[3]
        blocks = linv.shape[1]
        chunk = nodes // parts
        tab_f, tab_b = tables(parts)
        vm = pltpu.VMEM
        dma = pltpu.SemaphoreType.DMA
        scratch = [
            vm((6, 2, modes, nodes), F32),
            vm((6, 2, modes, nodes), BF16),
            vm((6, parts, 2, modes, chunk), BF16),
            vm((NPHI, 2 * M), BF16),
            vm((2 * M, NPHI), BF16),
            vm((3, parts, 2, modes, chunk), BF16),
            vm((3, 2, modes, nodes), BF16),
            vm((2 * modes, nodes), BF16),
            vm((modes, blocks, 128, 128), BF16),
            vm((modes, 128, nodes), BF16),
            vm((modes, 128, 128), BF16),
            vm((modes, 128, 128), BF16),
            vm((modes, 128, 128), BF16),
            vm((2, modes, 128), F32),
            vm((1, 2, 128), jnp.int32),
            vm((128, 128), BF16),
            vm((128, 128), BF16),
            vm((modes, 2, 128), F32),
            vm((modes, 2, 128), F32),
            vm((2 * modes, 128), F32),
            vm((places, 128, 128), BF16),
            vm((places, 128, 128), BF16),
            vm((places, 2, 128), F32),
            vm((places, 2, 128), F32),
            vm((places, 4, 128), F32),
            vm((modes, 4, 128), F32),
            vm((2 * modes, nodes), BF16),
            dma((6,)), dma((6,)), dma((modes,)), dma((modes,)),
            dma((2, parts - 1)), dma((2, parts - 1)),
            dma((3, parts - 1)), dma((3, parts - 1)),
            dma, dma, dma, dma, dma, dma, dma, dma, dma, dma,
        ]
        any_spec = pl.BlockSpec(memory_space=pl.ANY)

        def body(*refs):
            kernel(parts, places, *refs)

        shapes = ((3, 2, modes, nodes), (2 * modes, nodes), (2, modes, 128))
        held = pl.pallas_call(
            body,
            name="dynamo",
            out_shape=tuple(pltpu.VMEM(shape, F32) for shape in shapes),
            in_specs=[any_spec] * 10,
            out_specs=(pl.BlockSpec(memory_space=pltpu.VMEM),) * 3,
            scratch_shapes=scratch,
            compiler_params=pltpu.CompilerParams(
                collective_id=0, has_side_effects=True, vmem_limit_bytes=65_650_000
            ),
        )(vel, mag, linv, lcpl, sinv, scpl, ssrc, rows, tab_f, tab_b)
        nl, az, sol = pl.pallas_call(
            put_out,
            name="put_out",
            out_shape=tuple(jax.ShapeDtypeStruct(shape, F32) for shape in shapes),
            in_specs=[pl.BlockSpec(memory_space=pltpu.VMEM)] * 3,
            out_specs=(any_spec,) * 3,
            scratch_shapes=[dma((3,))],
            compiler_params=pltpu.CompilerParams(has_side_effects=True, vmem_limit_bytes=60 * 2**20),
        )(*[pltpu.with_memory_space_constraint(a, pltpu.VMEM) for a in held])
        return nl, az.reshape(2, modes, nodes), sol

    return jax.shard_map(shards, mesh=mesh, in_specs=in_specs, out_specs=out_specs, check_vma=False)
```

```python
import jax
import jax.numpy as jnp
import numpy as np
from jax import lax
from jax.experimental import pallas as pl
from jax.experimental.pallas import tpu as pltpu
from jax.sharding import PartitionSpec as P

M = 64
NPHI = 192
DT = 0.5
MESH = pl.DeviceIdType.MESH
F32 = jnp.float32
BF16 = jnp.bfloat16

SLOT_OF = ((0, 0), (0, 2), (1, 0), (1, 2), (0, 1), (1, 1))
VR, VZ, BR, BZ, VP, BP = range(6)


def tables(parts):
    local = M // parts
    k = np.arange(NPHI)[:, None]
    m = np.arange(M)[None, :]
    phase = ((k * m) % NPHI) * (2.0 * np.pi / NPHI)
    both = np.stack([np.cos(phase), np.sin(phase)])
    both = both.reshape(2, NPHI, parts, local).transpose(1, 2, 0, 3).reshape(NPHI, 2 * M)
    weights = np.where(np.arange(M) == 0, 1.0, 2.0) / NPHI
    w = np.broadcast_to(weights.reshape(parts, 1, local), (parts, 2, local)).reshape(2 * M)
    return jnp.asarray(both, BF16), jnp.asarray((both * w).T, BF16)


def dot(a, b):
    return jnp.dot(a, b, preferred_element_type=F32)


def dot_nt(a, b):
    return lax.dot_general(a, b, (((1,), (1,)), ((), ())), preferred_element_type=F32)


def level_of(q, levels):
    return levels + 1 if q == 0 else (q & -q).bit_length()


def parent_of(q, levels):
    level = level_of(q, levels)
    if level == levels:
        return 0
    return (q >> (level + 1) << (level + 1)) + 2**level


def kernel(
    parts, places,
    vel, mag, linv, lcpl, sinv, scpl, ssrc, rows, tab_f, tab_b,
    nl32, az, sol,
    stage, vb, xr, tf, tb, nb, nr, src16, lin, gup, gt, smat, cmat, hmat, ssv, rowv, pt0, p1,
    srcb, ubuf, urow, hs, ss, srcs, us, xo, xin, ls,
    sem_vb, sem_small, sem_lin, sem_g, sem_s1, sem_r1, sem_s2, sem_r2,
    sem_ss, sem_sh, sem_sc, sem_rs, sem_rh, sem_rc, sem_us, sem_ur, sem_xs, sem_xr,
):
    modes = src16.shape[0] // 2
    nodes = src16.shape[1]
    chunk = nodes // parts
    blocks = lin.shape[1]
    levels = places.bit_length() - 1
    y = lax.axis_index("mode")
    me = lax.axis_index("mesh")
    solver = lax.rem(me, 2) == 1
    together = 4

    def lanes_of(part):
        return pl.ds(pl.multiple_of(part * chunk, 128), chunk)

    def drain(ref, sem):
        pltpu.make_async_copy(ref, ref, sem).wait()

    for slot, (which, comp) in enumerate(SLOT_OF):
        pltpu.make_async_copy((vel, mag)[which].at[comp], stage.at[slot], sem_vb.at[slot // 4]).start()
    barrier = pltpu.get_barrier_semaphore()

    def greet(i, carry):
        other = jnp.where(me + i >= places, me + i - places, me + i)
        pl.semaphore_signal(barrier, inc=1, device_id=(y, other), device_id_type=MESH)
        return carry

    for d in range(1, parts):
        pl.semaphore_signal(barrier, inc=1, device_id=(lax.rem(y + d, parts), me), device_id_type=MESH)
    lax.fori_loop(1, places, greet, 0)

    small = ((sinv, smat), (scpl, cmat), (ssrc, ssv), (rows, rowv), (tab_f, tf), (tab_b, tb))
    for i, (a, b) in enumerate(small):
        pltpu.make_async_copy(a, b, sem_small.at[i]).start()

    drain(stage.at[:4], sem_vb.at[0])
    for slot in range(4):
        vb[slot] = stage[slot].astype(BF16)
    for i, (a, b) in enumerate(small):
        drain(b, sem_small.at[i])

    srow = lax.broadcasted_iota(jnp.int32, (128, 128), 0)
    pt0[...] = (srow == jnp.broadcast_to(rowv[0, 0:1, :], (128, 128))).astype(F32).astype(BF16)
    p1[...] = (srow == jnp.broadcast_to(rowv[0, 1:2, :], (128, 128))).astype(F32).T.astype(BF16)

    def build_h(m, carry):
        coupling = dot(p1[...], cmat[m]).astype(BF16)
        hmat[m] = dot(coupling, smat[m]).astype(BF16)
        return carry

    lax.fori_loop(0, modes // 4 * 3, build_h, 0, unroll=4)
    pl.semaphore_wait(barrier, parts - 1 + places - 1)

    def to_mode(src, dst, send, recv, other):
        return pltpu.make_async_remote_copy(
            src_ref=src, dst_ref=dst, send_sem=send, recv_sem=recv, device_id=(other, me), device_id_type=MESH
        )

    def exchange(group, lo, hi):
        for d in (2, 3, 1):
            other = lax.rem(y + d, parts)
            to_mode(
                vb.at[lo:hi, :, :, lanes_of(other)], xr.at[lo:hi, y],
                sem_s1.at[group], sem_r1.at[group, d - 1], other,
            ).start()
        for slot in range(lo, hi):
            xr[slot, y] = vb[slot, :, :, lanes_of(y)]

    def exchanged(group, lo, hi):
        for d in range(1, parts):
            drain(xr.at[lo:hi, 0], sem_r1.at[group, d - 1])

    exchange(0, 0, 4)

    def load_mode(m, carry):
        pltpu.make_async_copy(linv.at[m], lin.at[m], sem_lin.at[lax.div(m, together)]).start()
        pltpu.make_async_copy(lcpl.at[m], gup.at[m], sem_g.at[lax.div(m, together)]).start()
        return carry

    lax.fori_loop(0, modes, load_mode, 0)

    drain(stage.at[4:], sem_vb.at[1])
    for slot in range(4, 6):
        vb[slot] = stage[slot].astype(BF16)

    def for_solvers(act, own):
        def one(m, carry):
            there = 2 * m + 1
            pl.when(there != me)(lambda: act(m, there))
            pl.when(there == me)(lambda: own(m))
            return carry

        lax.fori_loop(0, modes, one, 0, unroll=4)

    def remote(src, dst, send, recv, there):
        return pltpu.make_async_remote_copy(
            src_ref=src, dst_ref=dst, send_sem=send, recv_sem=recv, device_id=(y, there), device_id_type=MESH
        )

    lax.fori_loop(modes // 4 * 3, modes, build_h, 0, unroll=4)
    for_solvers(
        lambda m, t: remote(smat.at[m], ss.at[me], sem_ss, sem_rs, t).start(),
        lambda m: pltpu.make_async_copy(smat.at[m], ss.at[me], sem_rs).start(),
    )
    srcb[...] = jnp.zeros_like(srcb)
    ubuf[...] = jnp.zeros_like(ubuf)
    for m in range(modes):
        for c in range(2):
            srcb[m, c : c + 1, :] = ssv[c, m : m + 1, :]
    for_solvers(
        lambda m, t: remote(hmat.at[m], hs.at[me], sem_sh, sem_rh, t).start(),
        lambda m: pltpu.make_async_copy(hmat.at[m], hs.at[me], sem_rh).start(),
    )
    for_solvers(
        lambda m, t: remote(srcb.at[m], srcs.at[me], sem_sc, sem_rc, t).start(),
        lambda m: pltpu.make_async_copy(srcb.at[m], srcs.at[me], sem_rc).start(),
    )

    zero = jnp.zeros((128, 128), BF16)

    def build_g(i, carry):
        these = pl.ds(i * together, together)
        drain(lin.at[these], sem_lin.at[i])
        drain(gup.at[these], sem_g.at[i])
        for j in range(together):
            m = i * together + j
            for b in range(0, blocks, 2):
                at = slice(b * 128, (b + 2) * 128)
                both = jnp.concatenate(
                    [jnp.concatenate([lin[m, b], zero], 1), jnp.concatenate([zero, lin[m, b + 1]], 1)], 0
                )
                made = dot(gup[m, :, at], both).astype(BF16)
                gup[m, :, at] = made
                gt[i * (together // 2) + j // 2, at, (j % 2) * 128 : (j % 2 + 1) * 128] = made.T
        return carry

    lax.fori_loop(0, 1, build_g, 0)
    lax.fori_loop(1, modes // together, build_g, 0)

    def transform(jobs):
        at = 0
        while at < chunk:
            width = min(256, chunk - at)
            here = slice(at, at + width)
            need = sorted({s for _, pairs in jobs for s in pairs})
            phys = {s: dot(tf[...], xr[s, :, :, :, here].reshape(2 * M, width)) for s in need}
            for comp, (a, b, c, d) in jobs:
                crossed = phys[a] * phys[b] - phys[c] * phys[d]
                back = dot(tb[...], crossed.astype(BF16)).astype(BF16)
                nb[comp, :, :, :, here] = back.reshape(parts, 2, modes, width)
            at += width

    def give_back(group, comp):
        for d in (2, 3, 1):
            other = lax.rem(y + d, parts)
            to_mode(
                nb.at[comp, other], nr.at[comp, :, :, lanes_of(y)],
                sem_s2.at[group], sem_r2.at[group, d - 1], other,
            ).start()
        nr[comp, :, :, lanes_of(y)] = nb[comp, y]

    exchanged(0, 0, 4)
    transform([(1, (VZ, BR, VR, BZ))])
    give_back(0, 1)

    mode_of = lax.rem(lax.broadcasted_iota(jnp.int32, (2 * modes, 128), 0), modes)
    leaf_update = jnp.zeros((2 * modes, 128), F32)
    for d in (0, 3, 1, 2):
        here = lanes_of(lax.rem(y + parts - d, parts))
        if d:
            drain(nb.at[1, 0], sem_r2.at[0, d - 1])
        source = stage[BP, :, :, here] + DT * nr[1, :, :, here].astype(F32)
        own = source.astype(BF16).reshape(2 * modes, chunk)
        src16[:, here] = own

        for i in range(modes // 2):
            got = dot(own, gt[i, here, :])
            for j in range(2):
                leaf_update += jnp.where(mode_of == 2 * i + j, got[:, j * 128 : (j + 1) * 128], 0.0)
        if d == 1:
            exchange(1, 4, 6)
    nl32[1] = nr[1].astype(F32)
    urow[...] = dot(leaf_update.astype(BF16), pt0[...])
    for m in range(modes):
        for c in range(2):
            ubuf[m, c : c + 1, :] = urow[c * modes + m : c * modes + m + 1, :]
    for_solvers(
        lambda m, t: remote(ubuf.at[m], us.at[me], sem_us, sem_ur, t).start(),
        lambda m: pltpu.make_async_copy(ubuf.at[m], us.at[me], sem_ur).start(),
    )

    def pair_at(b):
        return pl.ds(pl.multiple_of(b * 256, 256), 256)

    low = lax.broadcasted_iota(jnp.int32, (2 * modes, 256), 1) < 128

    def leaf_forward(b, carry):
        own = src16[:, pair_at(b)].astype(F32)
        own = jnp.concatenate([jnp.where(low, own, 0.0), jnp.where(low, 0.0, own)], 0).astype(BF16)
        left = right = jnp.zeros((2 * modes, 128), F32)
        for m in range(modes):
            got = dot_nt(own, jnp.concatenate([lin[m, 2 * b], lin[m, 2 * b + 1]], 1))
            left = jnp.where(mode_of == m, got[: 2 * modes], left)
            right = jnp.where(mode_of == m, got[2 * modes :], right)
        ls[:, pair_at(b)] = jnp.concatenate([left, right], 1).astype(BF16)
        return carry

    lax.fori_loop(0, blocks // 2, leaf_forward, 0, unroll=2)

    exchanged(1, 4, 6)
    transform([(0, (VP, BZ, VZ, BP)), (2, (VR, BP, VP, BR))])
    give_back(1, 0)
    give_back(2, 2)

    @pl.when(solver)
    def _():
        drain(hs, sem_rh)
        drain(srcs, sem_rc)
        drain(us, sem_ur)
        drain(ss, sem_rs)
        ranked = [[q for q in range(places) if level_of(q, levels) == k] for k in range(levels + 2)]
        top = places // 2
        none = jnp.zeros((2, 128), F32)

        def side(a, b):
            return jnp.concatenate([a, b], 1)

        def g_of(q, arrived):
            return srcs[q] - arrived

        joined = dot(ss[0], hs[top]).astype(BF16)
        g, w, x = {}, {}, {}
        arrived = {q: us[q - 1] + us[q] for q in ranked[1]}
        reduced = {}

        def pairs(level):
            return list(zip(ranked[level][::2], ranked[level][1::2]))

        def up(level):
            for a, b in pairs(level):
                g[a], g[b] = g_of(a, arrived[a]), g_of(b, arrived[b])
                arrived[(a + b) // 2] = dot_nt(side(g[a], g[b]).astype(BF16), side(hs[a], hs[b]))

        def reduce_pairs(level):
            for a, b in pairs(level):
                rows_ab = jnp.concatenate([side(g[a], none), side(none, g[b])], 0).astype(BF16)
                reduced[a] = dot_nt(rows_ab, side(ss[a], ss[b])).astype(BF16)

        def back_pairs(level):
            for a, b in pairs(level):
                got = dot(reduced[a], side(ss[a], ss[b]))
                w[a], w[b] = got[:2, :128], got[2:, 128:]

        for level in range(1, levels):
            up(level)
            if level > 1:
                back_pairs(level - 1)
            reduce_pairs(level)
        g_top = g_of(top, arrived[top]).astype(BF16)
        reduced_top = dot_nt(g_top, ss[top]).astype(BF16).astype(F32)
        reduced_0 = (dot_nt(srcs[0].astype(BF16), ss[0]) - dot_nt(g_top, joined)).astype(BF16)
        back_pairs(levels - 1)
        x[top] = dot(
            side(reduced_top, -reduced_0.astype(F32)).astype(BF16), jnp.concatenate([ss[top], joined], 0)
        )
        for level in range(levels - 1, 0, -1):
            for a, b in zip(ranked[level][::2], ranked[level][1::2]):
                got = dot(x[parent_of(a, levels)].astype(BF16), side(hs[a], hs[b]))
                x[a], x[b] = w[a] - got[:, :128], w[b] - got[:, 128:]
        x[0] = dot(reduced_0, ss[0])
        for p in range(places):
            xo[p, 0:2, :] = x[p]
            xo[p, 2:4, :] = x[2 * (p // 2) + 1]

        def send(p, carry):
            def away():
                pltpu.make_async_remote_copy(
                    src_ref=xo.at[p], dst_ref=xin.at[lax.div(me, 2)], send_sem=sem_xs, recv_sem=sem_xr,
                    device_id=(y, p), device_id_type=MESH,
                ).start()

            pl.when(p != me)(away)
            pl.when(p == me)(lambda: pltpu.make_async_copy(xo.at[p], xin.at[lax.div(me, 2)], sem_xr).start())
            return carry

        lax.fori_loop(0, places, send, 0, unroll=8)

    mode_col = jnp.concatenate([mode_of, mode_of], 0)

    def stacked(rows, which):
        rows = rows.astype(F32)
        return jnp.concatenate([jnp.where(which == m, rows, 0.0).astype(BF16) for m in range(modes)], 1)

    def leaf_back(b, carry):
        own = ls[:, pair_at(b)]
        own = stacked(jnp.concatenate([own[:, :128], own[:, 128:]], 0), mode_col)
        both = jnp.concatenate(
            [jnp.concatenate([lin[m, 2 * b], lin[m, 2 * b + 1]], 1) for m in range(modes)], 0
        )
        got = dot(own, both)
        az[:, pair_at(b)] = jnp.concatenate([got[: 2 * modes, :128], got[2 * modes :, 128:]], 1)
        return carry

    lax.fori_loop(0, blocks // 2, leaf_back, 0, unroll=5)

    for group, (lo, hi) in enumerate(((0, 4), (4, 6))):
        drain(xr.at[lo:hi, : parts - 1], sem_s1.at[group])
    for group in range(3):
        drain(nb.at[0, : parts - 1], sem_s2.at[group])

    def sent(count):
        drain(hmat.at[:count], sem_sh)
        drain(smat.at[:count], sem_ss)
        drain(srcb.at[:count], sem_sc)
        drain(ubuf.at[:count], sem_us)

    @pl.when(solver)
    def _():
        sent(modes - 1)
        drain(xo.at[: places - 1], sem_xs)

    pl.when(jnp.logical_not(solver))(lambda: sent(modes))

    drain(xin, sem_xr)
    for m in range(modes):
        for c in range(2):
            urow[c * modes + m : c * modes + m + 1, :] = xin[m, 2 + c : 3 + c, :]
    above = dot_nt(urow[...].astype(BF16), pt0[...]).astype(BF16)

    above = stacked(above, mode_of)
    for b in range(blocks // 2):
        at = slice(b * 256, (b + 1) * 256)
        az[:, at] -= dot(above, gup[:, :, at].reshape(modes * 128, 256))
    for comp in (0, 2):
        for d in range(1, parts):
            drain(nb.at[comp, 0], sem_r2.at[1 + comp // 2, d - 1])
        nl32[comp] = nr[comp].astype(F32)
    for m in range(modes):
        for c in range(2):
            sol[c, m : m + 1, :] = xin[m, c : c + 1, :]


def put_out(*refs):
    moves = [pltpu.make_async_copy(refs[i], refs[3 + i], refs[6].at[i]) for i in range(3)]
    for move in moves:
        move.start()
    for move in moves:
        move.wait()


def solution(mesh):
    parts, places = mesh.shape["mode"], mesh.shape["mesh"]
    in_specs = (
        P(None, None, "mode", "mesh"),
        P(None, None, "mode", "mesh"),
        P("mode", "mesh", None, None),
        P("mode", None, "mesh"),
        P("mode", "mesh", None),
        P("mode", "mesh", None),
        P(None, "mode", "mesh"),
        P("mesh", None, None),
    )
    out_specs = (P(None, None, "mode", "mesh"), P(None, "mode", "mesh"), P(None, "mode", "mesh"))

    def shards(vel, mag, linv, lcpl, sinv, scpl, ssrc, rows):
        modes, nodes = vel.shape[2], vel.shape[3]
        blocks = linv.shape[1]
        chunk = nodes // parts
        tab_f, tab_b = tables(parts)
        vm = pltpu.VMEM
        dma = pltpu.SemaphoreType.DMA
        scratch = [
            vm((6, 2, modes, nodes), F32),
            vm((6, 2, modes, nodes), BF16),
            vm((6, parts, 2, modes, chunk), BF16),
            vm((NPHI, 2 * M), BF16),
            vm((2 * M, NPHI), BF16),
            vm((3, parts, 2, modes, chunk), BF16),
            vm((3, 2, modes, nodes), BF16),
            vm((2 * modes, nodes), BF16),
            vm((modes, blocks, 128, 128), BF16),
            vm((modes, 128, nodes), BF16),
            vm((modes // 2, nodes, 256), BF16),
            vm((modes, 128, 128), BF16),
            vm((modes, 128, 128), BF16),
            vm((modes, 128, 128), BF16),
            vm((2, modes, 128), F32),
            vm((1, 2, 128), jnp.int32),
            vm((128, 128), BF16),
            vm((128, 128), BF16),
            vm((modes, 2, 128), F32),
            vm((modes, 2, 128), F32),
            vm((2 * modes, 128), F32),
            vm((places, 128, 128), BF16),
            vm((places, 128, 128), BF16),
            vm((places, 2, 128), F32),
            vm((places, 2, 128), F32),
            vm((places, 4, 128), F32),
            vm((modes, 4, 128), F32),
            vm((2 * modes, nodes), BF16),
            dma((2,)), dma((6,)), dma((4,)), dma((4,)),
            dma((2,)), dma((2, parts - 1)),
            dma((3,)), dma((3, parts - 1)),
            dma, dma, dma, dma, dma, dma, dma, dma, dma, dma,
        ]
        any_spec = pl.BlockSpec(memory_space=pl.ANY)

        def body(*refs):
            kernel(parts, places, *refs)

        shapes = ((3, 2, modes, nodes), (2 * modes, nodes), (2, modes, 128))
        held = pl.pallas_call(
            body,
            name="dynamo",
            out_shape=tuple(pltpu.VMEM(shape, F32) for shape in shapes),
            in_specs=[any_spec] * 10,
            out_specs=(pl.BlockSpec(memory_space=pltpu.VMEM),) * 3,
            scratch_shapes=scratch,
            compiler_params=pltpu.CompilerParams(
                collective_id=0, has_side_effects=True, vmem_limit_bytes=65_650_000
            ),
        )(vel, mag, linv, lcpl, sinv, scpl, ssrc, rows, tab_f, tab_b)
        nl, az, sol = pl.pallas_call(
            put_out,
            name="put_out",
            out_shape=tuple(jax.ShapeDtypeStruct(shape, F32) for shape in shapes),
            in_specs=[pl.BlockSpec(memory_space=pltpu.VMEM)] * 3,
            out_specs=(any_spec,) * 3,
            scratch_shapes=[dma((3,))],
            compiler_params=pltpu.CompilerParams(has_side_effects=True, vmem_limit_bytes=60 * 2**20),
        )(*[pltpu.with_memory_space_constraint(a, pltpu.VMEM) for a in held])
        return nl, az.reshape(2, modes, nodes), sol

    return jax.shard_map(shards, mesh=mesh, in_specs=in_specs, out_specs=out_specs, check_vma=False)
```

```python
import jax
import jax.numpy as jnp
import numpy as np
from jax import lax
from jax.experimental import pallas as pl
from jax.experimental.pallas import tpu as pltpu
from jax.sharding import PartitionSpec as P

M = 64
NPHI = 192
DT = 0.5
MESH = pl.DeviceIdType.MESH
F32 = jnp.float32
BF16 = jnp.bfloat16

SLOT_OF = ((0, 0), (0, 2), (1, 0), (1, 2), (0, 1), (1, 1))
VR, VZ, BR, BZ, VP, BP = range(6)


def tables(parts):
    local = M // parts
    k = np.arange(NPHI)[:, None]
    m = np.arange(M)[None, :]
    phase = ((k * m) % NPHI) * (2.0 * np.pi / NPHI)
    both = np.stack([np.cos(phase), np.sin(phase)])
    both = both.reshape(2, NPHI, parts, local).transpose(1, 2, 0, 3).reshape(NPHI, 2 * M)
    weights = np.where(np.arange(M) == 0, 1.0, 2.0) / NPHI
    w = np.broadcast_to(weights.reshape(parts, 1, local), (parts, 2, local)).reshape(2 * M)
    return jnp.asarray(both, BF16), jnp.asarray((both * w).T, BF16)


def dot(a, b):
    return jnp.dot(a, b, preferred_element_type=F32)


def dot_nt(a, b):
    return lax.dot_general(a, b, (((1,), (1,)), ((), ())), preferred_element_type=F32)


def level_of(q, levels):
    return levels + 1 if q == 0 else (q & -q).bit_length()


def parent_of(q, levels):
    level = level_of(q, levels)
    if level == levels:
        return 0
    return (q >> (level + 1) << (level + 1)) + 2**level


def kernel(
    parts, places,
    vel, mag, linv, lcpl, sinv, scpl, ssrc, rows, tab_f, tab_b,
    nl32, az, sol,
    stage, vb, xr, tf, tb, nb, nr, src16, lin, gup, gt, smat, cmat, hmat, ssv, rowv, pt0, p1,
    srcb, ubuf, urow, hs, ss, srcs, us, xo, xin, ls,
    sem_vb, sem_small, sem_lin, sem_g, sem_s1, sem_r1, sem_s2, sem_r2,
    sem_ss, sem_sh, sem_sc, sem_rs, sem_rh, sem_rc, sem_us, sem_ur, sem_xs, sem_xr,
):
    modes = src16.shape[0] // 2
    nodes = src16.shape[1]
    chunk = nodes // parts
    blocks = lin.shape[1]
    levels = places.bit_length() - 1
    y = lax.axis_index("mode")
    me = lax.axis_index("mesh")
    solver = lax.rem(me, 2) == 1
    together = 4

    def lanes_of(part):
        return pl.ds(pl.multiple_of(part * chunk, 128), chunk)

    def drain(ref, sem):
        pltpu.make_async_copy(ref, ref, sem).wait()

    for slot, (which, comp) in enumerate(SLOT_OF):
        pltpu.make_async_copy((vel, mag)[which].at[comp], stage.at[slot], sem_vb.at[slot // 4]).start()
    barrier = pltpu.get_barrier_semaphore()

    def around(at, step, size):
        return jnp.where(at + step >= size, at + step - size, at + step)

    def far_first(size):
        return sorted(range(1, size), key=lambda i: -min(i, size - i))

    for step in far_first(places):
        other = around(me, step, places)
        pl.semaphore_signal(barrier, inc=1, device_id=(y, other), device_id_type=MESH)
    for d in range(1, parts):
        pl.semaphore_signal(barrier, inc=1, device_id=(lax.rem(y + d, parts), me), device_id_type=MESH)

    small = ((sinv, smat), (scpl, cmat), (ssrc, ssv), (rows, rowv), (tab_f, tf), (tab_b, tb))
    for i, (a, b) in enumerate(small):
        pltpu.make_async_copy(a, b, sem_small.at[i]).start()

    drain(stage.at[:4], sem_vb.at[0])
    for slot in range(4):
        vb[slot] = stage[slot].astype(BF16)
    for i, (a, b) in enumerate(small):
        drain(b, sem_small.at[i])

    srow = lax.broadcasted_iota(jnp.int32, (128, 128), 0)
    pt0[...] = (srow == jnp.broadcast_to(rowv[0, 0:1, :], (128, 128))).astype(F32).astype(BF16)
    p1[...] = (srow == jnp.broadcast_to(rowv[0, 1:2, :], (128, 128))).astype(F32).T.astype(BF16)

    def build_h(m, carry):
        coupling = dot(p1[...], cmat[m]).astype(BF16)
        hmat[m] = dot(coupling, smat[m]).astype(BF16)
        return carry

    lax.fori_loop(0, modes // 4 * 3, build_h, 0, unroll=4)
    pl.semaphore_wait(barrier, parts - 1 + places - 1)

    def to_mode(src, dst, send, recv, other):
        return pltpu.make_async_remote_copy(
            src_ref=src, dst_ref=dst, send_sem=send, recv_sem=recv, device_id=(other, me), device_id_type=MESH
        )

    def exchange(group, lo, hi):
        for d in (2, 3, 1):
            other = lax.rem(y + d, parts)
            to_mode(
                vb.at[lo:hi, :, :, lanes_of(other)], xr.at[lo:hi, y],
                sem_s1.at[group], sem_r1.at[group, d - 1], other,
            ).start()
        for slot in range(lo, hi):
            xr[slot, y] = vb[slot, :, :, lanes_of(y)]

    def exchanged(group, lo, hi):
        for d in range(1, parts):
            drain(xr.at[lo:hi, 0], sem_r1.at[group, d - 1])

    exchange(0, 0, 4)

    def load_mode(m, carry):
        pltpu.make_async_copy(linv.at[m], lin.at[m], sem_lin.at[lax.div(m, together)]).start()
        pltpu.make_async_copy(lcpl.at[m], gup.at[m], sem_g.at[lax.div(m, together)]).start()
        return carry

    lax.fori_loop(0, modes, load_mode, 0)

    drain(stage.at[4:], sem_vb.at[1])
    for slot in range(4, 6):
        vb[slot] = stage[slot].astype(BF16)

    def for_solvers(act, own):
        chip = lax.div(me, 2)
        for step in far_first(modes):
            m = around(chip, step, modes)
            act(m, 2 * m + 1)
        pl.when(solver)(lambda: own(chip))
        pl.when(jnp.logical_not(solver))(lambda: act(chip, me + 1))

    def remote(src, dst, send, recv, there):
        return pltpu.make_async_remote_copy(
            src_ref=src, dst_ref=dst, send_sem=send, recv_sem=recv, device_id=(y, there), device_id_type=MESH
        )

    lax.fori_loop(modes // 4 * 3, modes, build_h, 0, unroll=4)
    for_solvers(
        lambda m, t: remote(smat.at[m], ss.at[me], sem_ss, sem_rs, t).start(),
        lambda m: pltpu.make_async_copy(smat.at[m], ss.at[me], sem_rs).start(),
    )
    srcb[...] = jnp.zeros_like(srcb)
    ubuf[...] = jnp.zeros_like(ubuf)
    for m in range(modes):
        for c in range(2):
            srcb[m, c : c + 1, :] = ssv[c, m : m + 1, :]
    for_solvers(
        lambda m, t: remote(hmat.at[m], hs.at[me], sem_sh, sem_rh, t).start(),
        lambda m: pltpu.make_async_copy(hmat.at[m], hs.at[me], sem_rh).start(),
    )
    for_solvers(
        lambda m, t: remote(srcb.at[m], srcs.at[me], sem_sc, sem_rc, t).start(),
        lambda m: pltpu.make_async_copy(srcb.at[m], srcs.at[me], sem_rc).start(),
    )

    zero = jnp.zeros((128, 128), BF16)

    def build_g(i, carry):
        these = pl.ds(i * together, together)
        drain(lin.at[these], sem_lin.at[i])
        drain(gup.at[these], sem_g.at[i])
        for j in range(together):
            m = i * together + j
            for b in range(0, blocks, 2):
                at = slice(b * 128, (b + 2) * 128)
                both = jnp.concatenate(
                    [jnp.concatenate([lin[m, b], zero], 1), jnp.concatenate([zero, lin[m, b + 1]], 1)], 0
                )
                made = dot(gup[m, :, at], both).astype(BF16)
                gup[m, :, at] = made
                gt[i * (together // 2) + j // 2, at, (j % 2) * 128 : (j % 2 + 1) * 128] = made.T
        return carry

    lax.fori_loop(0, 1, build_g, 0)
    lax.fori_loop(1, modes // together, build_g, 0)

    def transform(jobs):
        at = 0
        while at < chunk:
            width = min(256, chunk - at)
            here = slice(at, at + width)
            need = sorted({s for _, pairs in jobs for s in pairs})
            phys = {s: dot(tf[...], xr[s, :, :, :, here].reshape(2 * M, width)) for s in need}
            for comp, (a, b, c, d) in jobs:
                crossed = phys[a] * phys[b] - phys[c] * phys[d]
                back = dot(tb[...], crossed.astype(BF16)).astype(BF16)
                nb[comp, :, :, :, here] = back.reshape(parts, 2, modes, width)
            at += width

    def give_back(group, comp):
        for d in (2, 3, 1):
            other = lax.rem(y + d, parts)
            to_mode(
                nb.at[comp, other], nr.at[comp, :, :, lanes_of(y)],
                sem_s2.at[group], sem_r2.at[group, d - 1], other,
            ).start()
        nr[comp, :, :, lanes_of(y)] = nb[comp, y]

    exchanged(0, 0, 4)
    transform([(1, (VZ, BR, VR, BZ))])
    give_back(0, 1)

    mode_of = lax.rem(lax.broadcasted_iota(jnp.int32, (2 * modes, 128), 0), modes)
    leaf_update = jnp.zeros((2 * modes, 128), F32)
    for d in (0, 3, 1, 2):
        here = lanes_of(lax.rem(y + parts - d, parts))
        if d:
            drain(nb.at[1, 0], sem_r2.at[0, d - 1])
        source = stage[BP, :, :, here] + DT * nr[1, :, :, here].astype(F32)
        own = source.astype(BF16).reshape(2 * modes, chunk)
        src16[:, here] = own

        for i in range(modes // 2):
            got = dot(own, gt[i, here, :])
            for j in range(2):
                leaf_update += jnp.where(mode_of == 2 * i + j, got[:, j * 128 : (j + 1) * 128], 0.0)
        if d == 1:
            exchange(1, 4, 6)
    nl32[1] = nr[1].astype(F32)
    urow[...] = dot(leaf_update.astype(BF16), pt0[...])
    for m in range(modes):
        for c in range(2):
            ubuf[m, c : c + 1, :] = urow[c * modes + m : c * modes + m + 1, :]
    for_solvers(
        lambda m, t: remote(ubuf.at[m], us.at[me], sem_us, sem_ur, t).start(),
        lambda m: pltpu.make_async_copy(ubuf.at[m], us.at[me], sem_ur).start(),
    )

    def pair_at(b):
        return pl.ds(pl.multiple_of(b * 256, 256), 256)

    low = lax.broadcasted_iota(jnp.int32, (2 * modes, 256), 1) < 128

    def leaf_forward(b, carry):
        own = src16[:, pair_at(b)].astype(F32)
        own = jnp.concatenate([jnp.where(low, own, 0.0), jnp.where(low, 0.0, own)], 0).astype(BF16)
        left = right = jnp.zeros((2 * modes, 128), F32)
        for m in range(modes):
            got = dot_nt(own, jnp.concatenate([lin[m, 2 * b], lin[m, 2 * b + 1]], 1))
            left = jnp.where(mode_of == m, got[: 2 * modes], left)
            right = jnp.where(mode_of == m, got[2 * modes :], right)
        ls[:, pair_at(b)] = jnp.concatenate([left, right], 1).astype(BF16)
        return carry

    lax.fori_loop(0, blocks // 2, leaf_forward, 0, unroll=2)

    exchanged(1, 4, 6)
    transform([(0, (VP, BZ, VZ, BP)), (2, (VR, BP, VP, BR))])
    give_back(1, 0)
    give_back(2, 2)

    @pl.when(solver)
    def _():
        drain(hs, sem_rh)
        drain(srcs, sem_rc)
        drain(us, sem_ur)
        drain(ss, sem_rs)
        ranked = [[q for q in range(places) if level_of(q, levels) == k] for k in range(levels + 2)]
        top = places // 2
        none = jnp.zeros((2, 128), F32)

        def side(a, b):
            return jnp.concatenate([a, b], 1)

        def g_of(q, arrived):
            return srcs[q] - arrived

        joined = dot(ss[0], hs[top]).astype(BF16)
        g, w, x = {}, {}, {}
        arrived = {q: us[q - 1] + us[q] for q in ranked[1]}
        reduced = {}

        def pairs(level):
            return list(zip(ranked[level][::2], ranked[level][1::2]))

        def up(level):
            for a, b in pairs(level):
                g[a], g[b] = g_of(a, arrived[a]), g_of(b, arrived[b])
                arrived[(a + b) // 2] = dot_nt(side(g[a], g[b]).astype(BF16), side(hs[a], hs[b]))

        def reduce_pairs(level):
            for a, b in pairs(level):
                rows_ab = jnp.concatenate([side(g[a], none), side(none, g[b])], 0).astype(BF16)
                reduced[a] = dot_nt(rows_ab, side(ss[a], ss[b])).astype(BF16)

        def back_pairs(level):
            for a, b in pairs(level):
                got = dot(reduced[a], side(ss[a], ss[b]))
                w[a], w[b] = got[:2, :128], got[2:, 128:]

        for level in range(1, levels):
            up(level)
            if level > 1:
                back_pairs(level - 1)
            reduce_pairs(level)
        g_top = g_of(top, arrived[top]).astype(BF16)
        reduced_top = dot_nt(g_top, ss[top]).astype(BF16).astype(F32)
        reduced_0 = (dot_nt(srcs[0].astype(BF16), ss[0]) - dot_nt(g_top, joined)).astype(BF16)
        back_pairs(levels - 1)
        x[top] = dot(
            side(reduced_top, -reduced_0.astype(F32)).astype(BF16), jnp.concatenate([ss[top], joined], 0)
        )
        for level in range(levels - 1, 0, -1):
            for a, b in zip(ranked[level][::2], ranked[level][1::2]):
                got = dot(x[parent_of(a, levels)].astype(BF16), side(hs[a], hs[b]))
                x[a], x[b] = w[a] - got[:, :128], w[b] - got[:, 128:]
        x[0] = dot(reduced_0, ss[0])
        for p in range(places):
            xo[p, 0:2, :] = x[p]
            xo[p, 2:4, :] = x[2 * (p // 2) + 1]

        mine = lax.div(me, 2)
        for step in far_first(places):
            p = around(me, step, places)
            remote(xo.at[p], xin.at[mine], sem_xs, sem_xr, p).start()
        pltpu.make_async_copy(xo.at[me], xin.at[mine], sem_xr).start()

    mode_col = jnp.concatenate([mode_of, mode_of], 0)

    def stacked(rows, which):
        rows = rows.astype(F32)
        return jnp.concatenate([jnp.where(which == m, rows, 0.0).astype(BF16) for m in range(modes)], 1)

    def leaf_back(b, carry):
        own = ls[:, pair_at(b)]
        own = stacked(jnp.concatenate([own[:, :128], own[:, 128:]], 0), mode_col)
        both = jnp.concatenate(
            [jnp.concatenate([lin[m, 2 * b], lin[m, 2 * b + 1]], 1) for m in range(modes)], 0
        )
        got = dot(own, both)
        az[:, pair_at(b)] = jnp.concatenate([got[: 2 * modes, :128], got[2 * modes :, 128:]], 1)
        return carry

    lax.fori_loop(0, blocks // 2, leaf_back, 0, unroll=5)

    for group, (lo, hi) in enumerate(((0, 4), (4, 6))):
        drain(xr.at[lo:hi, : parts - 1], sem_s1.at[group])
    for group in range(3):
        drain(nb.at[0, : parts - 1], sem_s2.at[group])

    def sent(count):
        drain(hmat.at[:count], sem_sh)
        drain(smat.at[:count], sem_ss)
        drain(srcb.at[:count], sem_sc)
        drain(ubuf.at[:count], sem_us)

    @pl.when(solver)
    def _():
        sent(modes - 1)
        drain(xo.at[: places - 1], sem_xs)

    pl.when(jnp.logical_not(solver))(lambda: sent(modes))

    drain(xin, sem_xr)
    for m in range(modes):
        for c in range(2):
            urow[c * modes + m : c * modes + m + 1, :] = xin[m, 2 + c : 3 + c, :]
    above = dot_nt(urow[...].astype(BF16), pt0[...]).astype(BF16)

    above = stacked(above, mode_of)
    for b in range(blocks // 2):
        at = slice(b * 256, (b + 1) * 256)
        az[:, at] -= dot(above, gup[:, :, at].reshape(modes * 128, 256))
    for comp in (0, 2):
        for d in range(1, parts):
            drain(nb.at[comp, 0], sem_r2.at[1 + comp // 2, d - 1])
        nl32[comp] = nr[comp].astype(F32)
    for m in range(modes):
        for c in range(2):
            sol[c, m : m + 1, :] = xin[m, c : c + 1, :]


def put_out(*refs):
    moves = [pltpu.make_async_copy(refs[i], refs[3 + i], refs[6].at[i]) for i in range(3)]
    for move in moves:
        move.start()
    for move in moves:
        move.wait()


def solution(mesh):
    parts, places = mesh.shape["mode"], mesh.shape["mesh"]
    in_specs = (
        P(None, None, "mode", "mesh"),
        P(None, None, "mode", "mesh"),
        P("mode", "mesh", None, None),
        P("mode", None, "mesh"),
        P("mode", "mesh", None),
        P("mode", "mesh", None),
        P(None, "mode", "mesh"),
        P("mesh", None, None),
    )
    out_specs = (P(None, None, "mode", "mesh"), P(None, "mode", "mesh"), P(None, "mode", "mesh"))

    def shards(vel, mag, linv, lcpl, sinv, scpl, ssrc, rows):
        modes, nodes = vel.shape[2], vel.shape[3]
        blocks = linv.shape[1]
        chunk = nodes // parts
        tab_f, tab_b = tables(parts)
        vm = pltpu.VMEM
        dma = pltpu.SemaphoreType.DMA
        scratch = [
            vm((6, 2, modes, nodes), F32),
            vm((6, 2, modes, nodes), BF16),
            vm((6, parts, 2, modes, chunk), BF16),
            vm((NPHI, 2 * M), BF16),
            vm((2 * M, NPHI), BF16),
            vm((3, parts, 2, modes, chunk), BF16),
            vm((3, 2, modes, nodes), BF16),
            vm((2 * modes, nodes), BF16),
            vm((modes, blocks, 128, 128), BF16),
            vm((modes, 128, nodes), BF16),
            vm((modes // 2, nodes, 256), BF16),
            vm((modes, 128, 128), BF16),
            vm((modes, 128, 128), BF16),
            vm((modes, 128, 128), BF16),
            vm((2, modes, 128), F32),
            vm((1, 2, 128), jnp.int32),
            vm((128, 128), BF16),
            vm((128, 128), BF16),
            vm((modes, 2, 128), F32),
            vm((modes, 2, 128), F32),
            vm((2 * modes, 128), F32),
            vm((places, 128, 128), BF16),
            vm((places, 128, 128), BF16),
            vm((places, 2, 128), F32),
            vm((places, 2, 128), F32),
            vm((places, 4, 128), F32),
            vm((modes, 4, 128), F32),
            vm((2 * modes, nodes), BF16),
            dma((2,)), dma((6,)), dma((4,)), dma((4,)),
            dma((2,)), dma((2, parts - 1)),
            dma((3,)), dma((3, parts - 1)),
            dma, dma, dma, dma, dma, dma, dma, dma, dma, dma,
        ]
        any_spec = pl.BlockSpec(memory_space=pl.ANY)

        def body(*refs):
            kernel(parts, places, *refs)

        shapes = ((3, 2, modes, nodes), (2 * modes, nodes), (2, modes, 128))
        held = pl.pallas_call(
            body,
            name="dynamo",
            out_shape=tuple(pltpu.VMEM(shape, F32) for shape in shapes),
            in_specs=[any_spec] * 10,
            out_specs=(pl.BlockSpec(memory_space=pltpu.VMEM),) * 3,
            scratch_shapes=scratch,
            compiler_params=pltpu.CompilerParams(
                collective_id=0, has_side_effects=True, vmem_limit_bytes=65_650_000
            ),
        )(vel, mag, linv, lcpl, sinv, scpl, ssrc, rows, tab_f, tab_b)
        nl, az, sol = pl.pallas_call(
            put_out,
            name="put_out",
            out_shape=tuple(jax.ShapeDtypeStruct(shape, F32) for shape in shapes),
            in_specs=[pl.BlockSpec(memory_space=pltpu.VMEM)] * 3,
            out_specs=(any_spec,) * 3,
            scratch_shapes=[dma((3,))],
            compiler_params=pltpu.CompilerParams(has_side_effects=True, vmem_limit_bytes=60 * 2**20),
        )(*[pltpu.with_memory_space_constraint(a, pltpu.VMEM) for a in held])
        return nl, az.reshape(2, modes, nodes), sol

    return jax.shard_map(shards, mesh=mesh, in_specs=in_specs, out_specs=out_specs, check_vma=False)
```
